8 devices in a mesh: rep: 1 (over z), dp: 8 (over x, y, core).
Axes of the slice: x: 2, y: 2, z: 1, core: 2. Of those that a mesh axis runs over, the one named last changes fastest.
Arguments:
- x: bfloat16 [8, 2048, 1280], P(('rep', 'dp'))
- dy: bfloat16 [8, 2048, 1280], P(('rep', 'dp'))
- w_gate: bfloat16 [2, 1280, 4480], replicated
- w_up: bfloat16 [2, 1280, 4480], replicated
- w_down: bfloat16 [2, 4480, 1280], replicated
- m_w_gate: float32 [2, 1280, 4480], P(None, 'dp')
- m_w_up: float32 [2, 1280, 4480], P(None, 'dp')
- m_w_down: float32 [2, 4480, 1280], P(None, 'dp')
- v_w_gate: float32 [2, 1280, 4480], P(None, 'dp')
- v_w_up: float32 [2, 1280, 4480], P(None, 'dp')
- v_w_down: float32 [2, 4480, 1280], P(None, 'dp')
Outputs:
- output 1: bfloat16 [2, 1280, 4480], P('rep')
- output 2: bfloat16 [2, 1280, 4480], P('rep')
- output 3: bfloat16 [2, 4480, 1280], P('rep')
- output 4: float32 [2, 1280, 4480], P('rep', 'dp')
- output 5: float32 [2, 1280, 4480], P('rep', 'dp')
- output 6: float32 [2, 4480, 1280], P('rep', 'dp')
- output 7: float32 [2, 1280, 4480], P('rep', 'dp')
- output 8: float32 [2, 1280, 4480], P('rep', 'dp')
- output 9: float32 [2, 4480, 1280], P('rep', 'dp')
All inputs are finite; a program needn't handle non-finite values.
Results may differ from the reference program's by a relative error of at most 0.022.
Values are sent between devices in bfloat16 or wider.
A program may use at most 2 GiB of HBM per device.

```python
import jax
import jax.numpy as jnp
from jax import lax

SEQUENCES = 8
TOKENS = 2048
D = 1280
FF = 4480
LAYERS = 2
NAMES = ("w_gate", "w_up", "w_down")
SHAPES = {"w_gate": (LAYERS, D, FF), "w_up": (LAYERS, D, FF), "w_down": (LAYERS, FF, D)}


def bump(key, n, height):
    away = (jnp.arange(n, dtype=jnp.int32) - jax.random.randint(key, (), 0, n, jnp.int32)) % n
    return jnp.where(away < n // 8, height, 1.0)


def together(key, own, strength):
    shared = jax.random.normal(key, own.shape[1:], jnp.float32)
    return (own + strength * shared) * lax.rsqrt(1 + strength * strength)


def setup_inputs(seed: int = 0, part: int = 0) -> dict:
    kx, kdy, ka, kb, kz, kf, kh, kl, *keys = jax.random.split(jax.random.key(seed), 8 + 3 * len(NAMES))
    kx, kdy, ka, kb = (jax.random.fold_in(k, part) for k in (kx, kdy, ka, kb))
    kw, km, kv = (keys[i::3] for i in range(3))
    shape = (SEQUENCES, TOKENS, D)
    much_x, much_dy = jax.random.uniform(kz, (2,), jnp.float32, 0.0, 1.0)
    loud = 2.0 ** jax.random.uniform(jax.random.fold_in(kz, 1), (), jnp.float32, -1.0, 2.0)
    layers = 2.0 ** jax.random.uniform(kl, (LAYERS, 1, 1), jnp.float32, -1.0, 1.0)
    x = together(ka, jax.random.normal(kx, shape, jnp.float32), much_x) * bump(kf, D, 4.0)
    dy = together(kb, jax.random.normal(kdy, shape, jnp.float32), much_dy)
    drawn = {"x": x.astype(jnp.bfloat16), "dy": (loud * dy * (SEQUENCES * TOKENS) ** -0.5).astype(jnp.bfloat16)}
    for key, name in zip(kw, NAMES, strict=True):
        w = jax.random.normal(key, SHAPES[name], jnp.float32) * SHAPES[name][1] ** -0.5
        drawn[name] = (w * {"w_gate": 1.0, "w_up": bump(kh, FF, 4.0), "w_down": layers}[name]).astype(jnp.bfloat16)
    for key, name in zip(km, NAMES, strict=True):
        drawn[f"m_{name}"] = 0.1 * jax.random.normal(key, SHAPES[name], jnp.float32)
    for key, name in zip(kv, NAMES, strict=True):
        drawn[f"v_{name}"] = jax.random.uniform(key, SHAPES[name], jnp.float32, 0.005, 0.015)
    return drawn


def matmul(a, w):
    return jnp.dot(a, w, preferred_element_type=jnp.float32).astype(jnp.bfloat16)


def normed(h):
    wide = h.astype(jnp.float32)
    scale = lax.rsqrt(jnp.mean(wide**2, -1, keepdims=True) + 1e-6)
    return (wide * scale).astype(jnp.bfloat16)


def layer(h, w):
    a = normed(h)
    gate = jnp.dot(a, w["w_gate"], preferred_element_type=jnp.float32)
    up = jnp.dot(a, w["w_up"], preferred_element_type=jnp.float32)
    return h + matmul((jax.nn.silu(gate) * up).astype(jnp.bfloat16), w["w_down"])


def adamw(w, m, v, g):
    m = 0.9 * m + 0.1 * g
    v = 0.95 * v + 0.05 * g * g
    step = m * lax.rsqrt(v + 1e-8) + 0.1 * w
    return (w - 0.02 * step).astype(jnp.bfloat16), m, v


def clipped(gradients, sum_of_squares, count):
    factor = jnp.minimum(1.0, 0.5 * lax.rsqrt(sum_of_squares / count + 1e-30))
    return [g * factor for g in gradients]


def stack(weights, h):
    return lax.scan(lambda h, w: (layer(h, w), None), h, weights)[0]


def reference(x, dy, w_gate, w_up, w_down, m_w_gate, m_w_up, m_w_down, v_w_gate, v_w_up, v_w_down):
    weights = dict(zip(NAMES, (w_gate, w_up, w_down), strict=True))

    def take(so_far, sequence):
        h, by_y = sequence
        _, back = jax.vjp(lambda w: stack(w, h), weights)
        return jax.tree.map(lambda total, term: total + term.astype(jnp.float32), so_far, back(by_y)[0]), None

    none_yet = {name: jnp.zeros(w.shape, jnp.float32) for name, w in weights.items()}
    by_weights, _ = lax.scan(take, none_yet, (x, dy))
    gradients = [by_weights[name].astype(jnp.bfloat16).astype(jnp.float32) for name in NAMES]
    gradients = clipped(gradients, sum(jnp.sum(g * g) for g in gradients), sum(g.size for g in gradients))
    new = [
        adamw(w.astype(jnp.float32), m, v, g)
        for w, m, v, g in zip((w_gate, w_up, w_down), (m_w_gate, m_w_up, m_w_down), (v_w_gate, v_w_up, v_w_down), gradients, strict=True)
    ]
    return tuple(one[which] for which in range(3) for one in new)
```

```python
import jax
import jax.numpy as jnp
from jax import lax
from jax.sharding import PartitionSpec as P

F32, BF16 = jnp.float32, jnp.bfloat16


def dot(a, b, dims):
    return lax.dot_general(a, b, (dims, ((), ())), preferred_element_type=F32)


def scale_of(h):
    wide = h.astype(F32)
    return wide, lax.rsqrt(jnp.mean(wide**2, -1, keepdims=True) + 1e-6)


def forward(h, wg, wu):
    wide, scale = scale_of(h)
    a = (wide * scale).astype(BF16)
    gate, up = dot(a, wg, ((1,), (0,))), dot(a, wu, ((1,), (0,)))
    return a, gate, up, (jax.nn.silu(gate) * up).astype(BF16)


def hidden_back(d_act, gate, up):
    d = d_act.astype(F32)
    s = jax.nn.sigmoid(gate)
    d_up = d * (gate * s)
    d_gate = d * up * (s * (1.0 + gate * (1.0 - s)))
    return d_gate.astype(BF16), d_up.astype(BF16)


def norm_back(h, da, dh):
    wide, scale = scale_of(h)
    da = da.astype(F32)
    along = jnp.sum(da * wide, -1, keepdims=True)
    d_wide = da * scale - wide * (along * scale**3 / h.shape[-1])
    return dh + d_wide.astype(BF16)


def adamw(w, m, v, g):
    m = 0.9 * m + 0.1 * g
    v = 0.95 * v + 0.05 * g * g
    step = m * lax.rsqrt(v + 1e-8) + 0.1 * w
    return (w - 0.02 * step).astype(BF16), m, v


def solution(mesh):
    n = mesh.shape["dp"]

    def scatter(g):
        return lax.psum_scatter(g.astype(BF16), "dp", scatter_dimension=0, tiled=True)

    def device_step(x, dy, wg, wu, wd, mg, mu, md, vg, vu, vd):
        x, dy = x[0], dy[0]
        T, N, M = ((0,), (0,)), ((1,), (0,)), ((1,), (1,))
        a0, gate0, up0, act0 = forward(x, wg[0], wu[0])
        h1 = x + dot(act0, wd[0], N).astype(BF16)
        a1, gate1, up1, act1 = forward(h1, wg[1], wu[1])
        gd1 = scatter(dot(act1, dy, T))
        dact1 = dot(dy, wd[1], M).astype(BF16)
        dgate1, dup1 = hidden_back(dact1, gate1, up1)
        gg1 = scatter(dot(a1, dgate1, T))
        gu1 = scatter(dot(a1, dup1, T))
        da1 = dot(dgate1, wg[1], M).astype(BF16) + dot(dup1, wu[1], M).astype(BF16)
        dh1 = norm_back(h1, da1, dy)
        gd0 = scatter(dot(act0, dh1, T))
        dact0 = dot(dh1, wd[0], M).astype(BF16)
        dgate0, dup0 = hidden_back(dact0, gate0, up0)
        gg0 = scatter(dot(a0, dgate0, T))
        gu0 = scatter(dot(a0, dup0, T))
        grads = ((gg0, gg1), (gu0, gu1), (gd0, gd1))
        squares = sum(jnp.sum(jnp.square(g.astype(F32))) for pair in grads for g in pair)
        count = sum(g.size for pair in grads for g in pair) * n
        total = lax.psum(squares, "dp")
        factor = jnp.minimum(1.0, 0.5 * lax.rsqrt(total / count + 1e-30))
        me = lax.axis_index("dp")
        ws, ms, vs = [], [], []
        for pair, w, m, v in zip(grads, (wg, wu, wd), (mg, mu, md), (vg, vu, vd)):
            rows = m.shape[1]
            new = []
            for l in range(2):
                own = lax.dynamic_slice_in_dim(w[l], me * rows, rows, 0).astype(F32)
                new.append(adamw(own, m[l], v[l], pair[l].astype(F32) * factor))
            ws.append(jnp.stack([lax.all_gather(new[l][0], "dp", axis=0, tiled=True) for l in range(2)]))
            ms.append(jnp.stack([new[l][1] for l in range(2)]))
            vs.append(jnp.stack([new[l][2] for l in range(2)]))
        return (*ws, *ms, *vs)

    tokens, whole, rows = P(("rep", "dp"), None, None), P(None, None, None), P(None, "dp", None)
    return jax.shard_map(
        device_step,
        mesh=mesh,
        in_specs=(tokens,) * 2 + (whole,) * 3 + (rows,) * 6,
        out_specs=(P("rep", None, None),) * 3 + (P("rep", "dp", None),) * 6,
        check_vma=False,
    )
```
